64 devices in a mesh: parts: 4 (over x, y), data: 16 (over z, core).
Axes of the slice: x: 2, y: 2, z: 8, core: 2. Of those that a mesh axis runs over, the one named last changes fastest.
The devices are a block of a 4x4x8 slice.
Arguments:
- feats: bfloat16 [8192, 90], P('data')
- labels: int32 [8192], P('data')
- w_in: float32 [90, 128, 100], P(None, 'parts'), parts along dimension 1
- w_out: float32 [128, 100], P('parts'), parts along dimension 0
- mom_in: float32 [90, 128, 100], P(None, 'parts'), parts along dimension 1
- mom_out: float32 [128, 100], P('parts'), parts along dimension 0
Outputs:
- output 1: float32 [90, 128, 100], P(None, 'parts'), parts along dimension 1
- output 2: float32 [128, 100], P('parts'), parts along dimension 0
- output 3: float32 [90, 128, 100], P(None, 'parts'), parts along dimension 1
- output 4: float32 [128, 100], P('parts'), parts along dimension 0
- output 5: float32 [128], P('parts'), parts along dimension 0
There are 4 independent parts. The reference program is written for one: setup_inputs(seed, part) draws one part's arguments, and reference() takes and returns one part's arrays. A program takes and returns all parts, laid end to end along the dimension named above; an argument that names none is the same for every part.
All inputs are finite; a program needn't handle non-finite values.
Results may differ from the reference program's by a relative error of at most 0.001.
Values are sent between devices in bfloat16 or wider.
A program may use at most 768 MiB of HBM per device.

```python
import math
import jax
import jax.numpy as jnp
from jax import lax

D = 90
HIDDEN = 100
CHAINS = 32
ROWS_DEV = 512
GROUP = 16
LEAPS = 16
N_ROWS = ROWS_DEV * GROUP
STEP = 1.0 / math.sqrt(N_ROWS * (D + HIDDEN))
PRIOR_VAR = 1.0


def setup_inputs(seed: int = 0, part: int = 0) -> dict:
    key = jax.random.key(seed)
    key_mean, key_noise, key_rate, key_draw, key_part = jax.random.split(key, 5)
    centers = jax.random.normal(key_mean, (GROUP, 1, D), jnp.float32)
    noise = jax.random.normal(key_noise, (GROUP, ROWS_DEV, D), jnp.float32)
    feats = (centers + noise).reshape(N_ROWS, D).astype(jnp.bfloat16)
    rates = jax.random.randint(key_rate, (GROUP, 1), 50, 951)
    draws = jax.random.randint(key_draw, (GROUP, ROWS_DEV), 0, 1000)
    labels = (draws < rates).astype(jnp.int32).reshape(N_ROWS)
    part_key = jax.random.fold_in(key_part, part)
    key_w1, key_w2, key_m1, key_m2 = jax.random.split(part_key, 4)
    w_in = jax.random.normal(key_w1, (D, CHAINS, HIDDEN), jnp.float32) * (2.0 * D) ** -0.5
    w_out = jax.random.normal(key_w2, (CHAINS, HIDDEN), jnp.float32) * (1.5 * HIDDEN ** -0.5)
    mom_in = jax.random.normal(key_m1, (D, CHAINS, HIDDEN), jnp.float32)
    mom_out = jax.random.normal(key_m2, (CHAINS, HIDDEN), jnp.float32)
    return {'feats': feats, 'labels': labels, 'w_in': w_in, 'w_out': w_out, 'mom_in': mom_in, 'mom_out': mom_out}


def block_terms(x_rows, lab_rows, w_flat, w_out):
    pre_act = jnp.dot(x_rows, w_flat, preferred_element_type=jnp.float32).reshape(ROWS_DEV, CHAINS, HIDDEN)
    hidden_act = jnp.tanh(pre_act)
    logits = jnp.sum(hidden_act * w_out, axis=-1)
    residual = lab_rows[:, None] - jax.nn.sigmoid(logits)
    grad_out = jnp.sum(hidden_act * residual[:, :, None], axis=0)
    back_grad = (residual[:, :, None] * w_out * (1.0 - hidden_act * hidden_act)).astype(jnp.bfloat16)
    grad_in = jnp.dot(x_rows.T, back_grad.reshape(ROWS_DEV, CHAINS * HIDDEN), preferred_element_type=jnp.float32)
    return grad_in.reshape(D, CHAINS, HIDDEN), grad_out, logits


def log_post_grad(x_blocks, lab_blocks, w_in, w_out):
    w_flat = w_in.astype(jnp.bfloat16).reshape(D, CHAINS * HIDDEN)

    def row_block(acc_sum, block_in):
        grad_in, grad_out, logits = block_terms(block_in[0], block_in[1], w_flat, w_out)
        return (acc_sum[0] + grad_in, acc_sum[1] + grad_out), logits

    sums, logits = lax.scan(row_block, (jnp.zeros_like(w_in), jnp.zeros_like(w_out)), (x_blocks, lab_blocks))
    return sums[0] - w_in / PRIOR_VAR, sums[1] - w_out / PRIOR_VAR, logits


def reference(feats, labels, w_in, w_out, mom_in, mom_out):
    x_blocks = feats.reshape(GROUP, ROWS_DEV, D)
    lab_blocks = labels.astype(jnp.float32).reshape(GROUP, ROWS_DEV)
    grad_in, grad_out, logits = log_post_grad(x_blocks, lab_blocks, w_in, w_out)
    mom_in = mom_in + 0.5 * STEP * grad_in
    mom_out = mom_out + 0.5 * STEP * grad_out

    def leap_step(state_now, unused):
        pos_in, pos_out, vel_in, vel_out = state_now
        pos_in = pos_in + STEP * vel_in
        pos_out = pos_out + STEP * vel_out
        g_in, g_out, g_logits = log_post_grad(x_blocks, lab_blocks, pos_in, pos_out)
        return (pos_in, pos_out, vel_in + STEP * g_in, vel_out + STEP * g_out), None

    state_end, unused_out = lax.scan(leap_step, (w_in, w_out, mom_in, mom_out), None, length=LEAPS - 1)
    pos_in, pos_out, vel_in, vel_out = state_end
    pos_in = pos_in + STEP * vel_in
    pos_out = pos_out + STEP * vel_out
    grad_in, grad_out, logits = log_post_grad(x_blocks, lab_blocks, pos_in, pos_out)
    vel_in = vel_in + 0.5 * STEP * grad_in
    vel_out = vel_out + 0.5 * STEP * grad_out
    row_loss = jnp.sum(jax.nn.softplus(logits) - lab_blocks[:, :, None] * logits, axis=(0, 1))
    energy = row_loss + (jnp.sum(pos_in * pos_in, axis=(0, 2)) + jnp.sum(pos_out * pos_out, axis=1)) / (2.0 * PRIOR_VAR) + 0.5 * (jnp.sum(vel_in * vel_in, axis=(0, 2)) + jnp.sum(vel_out * vel_out, axis=1))
    return pos_in, pos_out, vel_in, vel_out, energy
```

```python
import functools
import math

import jax
import jax.numpy as jnp
from jax import lax
from jax.experimental import pallas as pl
from jax.experimental.pallas import tpu as pltpu
from jax.sharding import PartitionSpec as P

LEAPS = 16
PRIOR_VAR = 1.0
LANES = 128
CORES = 2
BLOCK = 8
CHUNKS = 4
F32 = jnp.float32
BF16 = jnp.bfloat16


def round_up(value, step):
    return -(-value // step) * step


def ring_gather(size, me, first, part, ring_send, ring_recv, pair_send, pair_recv):
    chips = size // CORES
    far = chips // 2
    pair = me + 1 - 2 * lax.rem(me, CORES)

    def at(steps):
        return lax.rem(me + CORES * steps + size, size)

    def ring_copy(way, step, q, src):
        owner = at(-way * step)
        slot = (1 - way) // 2
        return pltpu.make_async_remote_copy(src_ref=src, dst_ref=part(owner, q), send_sem=ring_send.at[slot, step, q], recv_sem=ring_recv.at[slot, step, q], device_id={'data': at(way)}, device_id_type=pl.DeviceIdType.MESH)

    def ring_wait(way, step, q):
        slot = (1 - way) // 2
        owner = at(-way * (step + 1))
        pltpu.make_async_remote_copy(src_ref=part(owner, q), dst_ref=part(owner, q), send_sem=ring_send.at[slot, step, q], recv_sem=ring_recv.at[slot, step, q], device_id={'data': me}, device_id_type=pl.DeviceIdType.MESH).wait_recv()

    def pair_copy(index, owner, q, src):
        return pltpu.make_async_remote_copy(src_ref=src, dst_ref=part(owner, q), send_sem=pair_send.at[index, q], recv_sem=pair_recv.at[index, q], device_id={'data': pair}, device_id_type=pl.DeviceIdType.MESH)

    def index_of(way, step):
        return step if way == 1 or step == far else chips - step

    sent = []
    pairs = []

    def goes(way, step, q):
        return step < far - 1 or (step == far - 1 and (q < CHUNKS // 2) == (way == 1))

    for q in range(CHUNKS):
        for way in (1, -1):
            if goes(way, 0, q):
                copy = ring_copy(way, 0, q, first(q))
                copy.start()
                sent.append(copy)
        copy = pair_copy(0, me, q, first(q))
        copy.start()
        sent.append(copy)
        pairs.append((0, q, copy))
    for step in range(1, far + 1):
        for q in range(CHUNKS):
            for way in (1, -1):
                if not goes(way, step - 1, q):
                    continue
                ring_wait(way, step - 1, q)
                owner = at(-way * step)
                if goes(way, step, q):
                    copy = ring_copy(way, step, q, part(owner, q))
                    copy.start()
                    sent.append(copy)
                copy = pair_copy(index_of(way, step), owner, q, part(owner, q))
                copy.start()
                sent.append(copy)
                pairs.append((index_of(way, step), q, copy))
    for index, q, copy in pairs:
        copy.wait_recv()
    for copy in sent:
        copy.wait_send()


def group_barrier(size, me):
    barrier = pltpu.get_barrier_semaphore()
    pair = me + 1 - 2 * lax.rem(me, CORES)
    for other in (pair, lax.rem(me + CORES, size), lax.rem(me + size - CORES, size)):
        pl.semaphore_signal(barrier, inc=1, device_id={'data': other}, device_id_type=pl.DeviceIdType.MESH)
    return barrier


def ring_sems(size):
    chips = size // CORES
    far = chips // 2
    return [pltpu.SemaphoreType.DMA((2, far, CHUNKS)), pltpu.SemaphoreType.DMA((2, far, CHUNKS)), pltpu.SemaphoreType.DMA((chips, CHUNKS)), pltpu.SemaphoreType.DMA((chips, CHUNKS))]


def rows_kernel(size, x_ref, y_ref, out_ref, *sems):
    me = lax.axis_index('data')
    barrier = group_barrier(size, me)
    num_feat, rows = x_ref.shape
    feat_pad = out_ref.shape[1]
    blocks = rows // LANES
    spare = jnp.zeros((feat_pad - num_feat - 1, LANES), F32)
    for i in range(blocks):
        feat = x_ref[:, pl.ds(i * LANES, LANES)].astype(F32)
        label = y_ref[pl.ds(i, 1), :].astype(F32)
        out_ref[me * blocks + i] = jnp.concatenate([feat, label, spare], axis=0).astype(BF16)
    pl.semaphore_wait(barrier, 3)
    per = blocks // CHUNKS

    def part(owner, q):
        return out_ref.at[pl.ds(owner * blocks + q * per, per)]

    ring_gather(size, me, lambda q: part(me, q), part, *sems)


def results_kernel(size, pos_ref, mom_ref, pos_all, mom_all, *sems):
    me = lax.axis_index('data')
    barrier = group_barrier(size, me)
    pos_all[:, me] = pos_ref[...]
    mom_all[:, me] = mom_ref[...]
    pl.semaphore_wait(barrier, 3)
    half = pos_ref.shape[0] // 2

    def own(q):
        ref = pos_ref if q % 2 == 0 else mom_ref
        return ref.at[pl.ds((q // 2) * half, half)]

    def part(owner, q):
        ref = pos_all if q % 2 == 0 else mom_all
        return ref.at[pl.ds((q // 2) * half, half), owner]

    ring_gather(size, me, own, part, *sems)


def chains_kernel(size, step_size, num_feat, hidden, w_hbm, mom_hbm, x_ref, w2_ref, mom2_ref, pos_out, mom_out, wst, pst, w2, p2, ys, acts, zpart, resid, logit, acc, gpart, w_in, mom_in, square, sem):
    me = lax.axis_index('data')
    mine = wst.shape[0]
    hid_pad, feat_pad = wst.shape[1:]
    total = x_ref.shape[0]
    slots = total // BLOCK
    tile = w_in.shape[1]
    half_step = 0.5 * step_size
    group = (me * mine) // tile
    row0 = lax.rem(me * mine, tile)
    copies = [pltpu.make_async_copy(src.at[:, pl.ds(pl.multiple_of(group * tile, tile), tile), :], dst, sem.at[i]) for i, (src, dst) in enumerate(((w_hbm, w_in), (mom_hbm, mom_in)))]
    for copy in copies:
        copy.start()
    for i in range(total):
        ys[pl.ds(i, 1), :] = x_ref[i, pl.ds(feat_pad - 16, 16), :].astype(F32)[num_feat - feat_pad + 16:num_feat - feat_pad + 17, :]
    acts[...] = jnp.zeros_like(acts)
    resid[...] = jnp.zeros_like(resid)
    acc[...] = jnp.zeros_like(acc)
    gpart[...] = jnp.zeros_like(gpart)
    square[...] = jnp.zeros_like(square)
    for copy in copies:
        copy.wait()
    lane_real = lax.broadcasted_iota(jnp.int32, (1, LANES), 1) < hidden
    for c in range(mine):
        for src, dst in ((w_in, wst), (mom_in, pst)):
            square[pl.ds(0, num_feat), pl.ds(0, hidden)] = src[:, row0 + c, :]
            dst[c] = square[...].T[:hid_pad, :feat_pad]
        for src, dst in ((w2_ref, w2), (mom2_ref, p2)):
            line = src[pl.ds(me * mine + c, 1), :]
            line = jnp.concatenate([line, jnp.zeros((1, LANES - hidden), F32)], axis=1)
            dst[c] = jnp.broadcast_to(line, (LANES, LANES)).T[:hid_pad, :]

    def rows(block, count):
        return jnp.concatenate([x_ref[block + i] for i in range(count)], axis=1)

    def forward(c, b, t, buf):
        block = b * BLOCK + 2 * t
        pre = jnp.dot(wst[c], rows(block, 2), preferred_element_type=F32)
        act = jnp.tanh(pre)
        acts[buf, :, pl.ds(2 * t * LANES, 2 * LANES)] = act
        out_w = w2[c]
        for h in range(2):
            term = act[:, h * LANES:(h + 1) * LANES] * out_w
            z = term[0:8]
            for j in range(1, hid_pad // 8):
                z = z + term[8 * j:8 * j + 8]
            zpart[buf, pl.ds((2 * t + h) * 8, 8), :] = z

    def residual(c, b, buf):
        z = zpart[buf, pl.ds(0, BLOCK, stride=8), :]
        for k in range(1, 8):
            z = z + zpart[buf, pl.ds(k, BLOCK, stride=8), :]
        logit[c, pl.ds(b * BLOCK, BLOCK), :] = z
        resid[buf] = ys[pl.ds(b * BLOCK, BLOCK), :] - jax.nn.sigmoid(z)

    def backward(c, b, t, buf, total_out):
        out_w = w2[c]
        back = []
        for h in range(2):
            act = acts[buf, :, pl.ds((2 * t + h) * LANES, LANES)]
            r = resid[buf, pl.ds(2 * t + h, 1), :]
            ra = r * act
            total_out = total_out + ra
            back.append((r - ra * act) * out_w)
        grad = lax.dot_general(jnp.concatenate(back, axis=1), rows(b * BLOCK + 2 * t, 2), (((1,), (1,)), ((), ())), preferred_element_type=F32)
        return grad, total_out

    def slot(now, before, grad):
        if before:
            total_out = acc[...] if before[1] else jnp.zeros_like(acc)
        for t in range(BLOCK // 2):
            if now:
                forward(*now[:2], t, now[2])
            if before:
                part, total_out = backward(*before[:2], t, before[2], total_out)
                grad = part if grad is None else grad + part
        if before:
            acc[...] = total_out
        if now:
            residual(*now)
        return grad

    feat_real = lax.broadcasted_iota(jnp.int32, (hid_pad, feat_pad), 1) < num_feat

    def update(c, grad, mom_step, pos_step):
        pos = wst[c]
        mom = pst[c] + mom_step * (jnp.where(feat_real, grad, 0.0) - pos / PRIOR_VAR)
        pst[c] = mom
        wst[c] = pos + pos_step * mom
        pos = w2[c]
        mom = p2[c] + mom_step * (jnp.sum(acc[...], axis=1, keepdims=True) - pos / PRIOR_VAR)
        p2[c] = mom
        w2[c] = pos + pos_step * mom

    def leap(index, carry):
        late = index == 0
        steps = {c: (jnp.where((index == 0) | (index == LEAPS), half_step, step_size), jnp.where(index == LEAPS, 0.0, step_size)) for c in range(mine - 1)}
        steps[mine - 1] = (jnp.where(index == 0, 0.0, jnp.where(index == 1, half_step, step_size)), jnp.where(index == 0, 0.0, step_size))
        count = 0
        before = (mine - 1, slots - 1, (mine * slots - 1) % 2)
        grad = gpart[...]
        for c in range(mine):
            for b in range(slots):
                now = (c, b, count % 2)
                grad = slot(now, before, grad)
                if before[1] == slots - 1:
                    update(before[0], grad, *steps[before[0]])
                    grad = None
                before = now
                count += 1
        gpart[...] = grad
        return carry

    lax.fori_loop(0, LEAPS + 1, leap, 0)
    grad = slot(None, (mine - 1, slots - 1, (mine * slots - 1) % 2), gpart[...])
    update(mine - 1, grad, half_step, 0.0)

    lane = lax.broadcasted_iota(jnp.int32, (1, LANES), 1)
    for c in range(mine):
        for src, dst in ((wst, pos_out), (pst, mom_out)):
            square[...] = jnp.zeros_like(square)
            square[pl.ds(0, hid_pad), pl.ds(0, feat_pad)] = src[c]
            dst[pl.ds(0, num_feat), c, :] = square[...].T[:num_feat, :]
        for src, dst in ((w2, pos_out), (p2, mom_out)):
            square[...] = jnp.zeros_like(square)
            square[pl.ds(0, hid_pad), :] = src[c]
            dst[pl.ds(num_feat, 1), c, :] = square[...].T[:1, :]
        z = logit[c]
        loss = jnp.maximum(z, 0.0) + jnp.log1p(jnp.exp(-jnp.abs(z))) - ys[...] * z
        energy = jnp.sum(loss, keepdims=True)
        prior = jnp.sum(wst[c] * wst[c], keepdims=True) + jnp.sum(w2[c][:, :1] * w2[c][:, :1], keepdims=True)
        kinetic = jnp.sum(pst[c] * pst[c], keepdims=True) + jnp.sum(p2[c][:, :1] * p2[c][:, :1], keepdims=True)
        energy = energy + prior / (2.0 * PRIOR_VAR) + 0.5 * kinetic
        pos_out[pl.ds(num_feat + 1, 1), c, :] = jnp.where(lane == 0, energy, 0.0)
        mom_out[pl.ds(num_feat + 1, 1), c, :] = jnp.zeros((1, LANES), F32)


def solution(mesh):
    size = mesh.shape['data']
    row_spec = P('data', None)
    label_spec = P('data')
    in_spec = P(None, 'parts', None)
    out_spec = P('parts', None)
    chain_spec = P('parts')
    vmem = pl.BlockSpec(memory_space=pltpu.VMEM)

    def run_chains(feats, labels, w_in, w_out, mom_in, mom_out):
        num_rows, num_feat = feats.shape
        hidden = w_in.shape[2]
        step_size = 1.0 / math.sqrt(num_rows * (num_feat + hidden))

        def device_body(x_rows, y_rows, w_in, w_out, mom_in, mom_out):
            chains = w_in.shape[1]
            mine = chains // size
            rows = x_rows.shape[0]
            feat_pad = round_up(num_feat + 1, 16)
            hid_pad = round_up(hidden, 8)
            blocks = num_rows // LANES
            gathered = pl.pallas_call(
                functools.partial(rows_kernel, size),
                out_shape=jax.ShapeDtypeStruct((blocks, feat_pad, LANES), BF16),
                in_specs=[vmem] * 2,
                out_specs=vmem,
                scratch_shapes=ring_sems(size),
                compiler_params=pltpu.CompilerParams(collective_id=0, has_side_effects=True),
            )(x_rows.T, y_rows.reshape(rows // LANES, LANES))
            tall = num_feat + 2
            square = round_up(max(feat_pad, hid_pad), LANES)
            pos, mom = pl.pallas_call(
                functools.partial(chains_kernel, size, step_size, num_feat, hidden),
                out_shape=(jax.ShapeDtypeStruct((tall, mine, LANES), F32),) * 2,
                in_specs=[pl.BlockSpec(memory_space=pl.ANY)] * 2 + [vmem] * 3,
                out_specs=(vmem,) * 2,
                scratch_shapes=[
                    pltpu.VMEM((mine, hid_pad, feat_pad), F32),
                    pltpu.VMEM((mine, hid_pad, feat_pad), F32),
                    pltpu.VMEM((mine, hid_pad, LANES), F32),
                    pltpu.VMEM((mine, hid_pad, LANES), F32),
                    pltpu.VMEM((blocks, LANES), F32),
                    pltpu.VMEM((2, hid_pad, BLOCK * LANES), F32),
                    pltpu.VMEM((2, BLOCK * 8, LANES), F32),
                    pltpu.VMEM((2, BLOCK, LANES), F32),
                    pltpu.VMEM((mine, blocks, LANES), F32),
                    pltpu.VMEM((hid_pad, LANES), F32),
                    pltpu.VMEM((hid_pad, feat_pad), F32),
                    pltpu.VMEM((num_feat, 8, hidden), F32),
                    pltpu.VMEM((num_feat, 8, hidden), F32),
                    pltpu.VMEM((square, square), F32),
                    pltpu.SemaphoreType.DMA((2,)),
                ],
                compiler_params=pltpu.CompilerParams(),
            )(w_in, mom_in, gathered, w_out, mom_out)
            pos_all, mom_all = pl.pallas_call(
                functools.partial(results_kernel, size),
                out_shape=(jax.ShapeDtypeStruct((tall, size, mine, LANES), F32),) * 2,
                in_specs=[vmem] * 2,
                out_specs=(vmem,) * 2,
                scratch_shapes=ring_sems(size),
                compiler_params=pltpu.CompilerParams(collective_id=1, has_side_effects=True),
            )(pos, mom)
            pos_all = pos_all.reshape(tall, chains, LANES)
            mom_all = mom_all.reshape(tall, chains, LANES)
            return pos_all[:num_feat, :, :hidden], pos_all[num_feat, :, :hidden], mom_all[:num_feat, :, :hidden], mom_all[num_feat, :, :hidden], pos_all[num_feat + 1, :, 0]

        mapped = jax.shard_map(device_body, mesh=mesh, in_specs=(row_spec, label_spec, in_spec, out_spec, in_spec, out_spec), out_specs=(in_spec, out_spec, in_spec, out_spec, chain_spec), check_vma=False)
        return mapped(feats, labels, w_in, w_out, mom_in, mom_out)

    return run_chains
```
